32 devices in a mesh: fsdp: 4 (over z), ctx: 4 (over y, x), tp: 2 (over core).
Axes of the slice: x: 2, y: 2, z: 4, core: 2. Of those that a mesh axis runs over, the one named last changes fastest.
Arguments:
- block_input: bfloat16 [4, 1024, 1600], P('fsdp', 'ctx'), may hold values from -8 to 8
- segments: int32 [4, 1024], P('fsdp', 'ctx'), may hold values from 0 to 3, never falling along the last dimension, each value on 1 to 512 neighbouring positions
- ln1_gain: float32 [1600], replicated, may hold values from 0.5 to 1.5
- ln1_shift: float32 [1600], replicated, may hold values from -3 to 3
- qkv_weight: bfloat16 [1600, 4800], P('fsdp'), may hold values from -4 to 4
- out_weight: bfloat16 [1600, 1600], P(None, 'fsdp'), may hold values from -0.4375 to 0.4375
- ln2_gain: float32 [1600], replicated, may hold values from 0.5 to 1.5
- ln2_shift: float32 [1600], replicated, may hold values from -3 to 3
- fc_weight: bfloat16 [1600, 6400], P('fsdp', 'tp'), may hold values from -0.15625 to 0.15625
- proj_weight: bfloat16 [6400, 1600], P('tp', 'fsdp'), may hold values from -0.078125 to 0.078125
- cotangent: bfloat16 [4, 1024, 1600], P('fsdp', 'ctx'), may hold values from -6 to 6
Outputs:
- block_output: bfloat16 [4, 1024, 1600], P('fsdp', 'ctx')
- grad_input: float32 [4, 1024, 1600], P('fsdp', 'ctx')
- grad_ln1_gain: float32 [1600], P(('fsdp', 'ctx'))
- grad_ln1_shift: float32 [1600], P(('fsdp', 'ctx'))
- grad_qkv_weight: float32 [1600, 4800], P(('fsdp', 'ctx'))
- grad_out_weight: float32 [1600, 1600], P(None, ('fsdp', 'ctx'))
- grad_ln2_gain: float32 [1600], P(('fsdp', 'ctx'))
- grad_ln2_shift: float32 [1600], P(('fsdp', 'ctx'))
- grad_fc_weight: float32 [1600, 6400], P(('fsdp', 'ctx'), 'tp')
- grad_proj_weight: float32 [6400, 1600], P('tp', ('fsdp', 'ctx'))
The draws below stay inside these ranges and needn't reach their ends.
All inputs are finite; a program needn't handle non-finite values.
Results may differ from the reference program's by a relative error of at most 0.013.
The reference program's roundings to bfloat16 on the way (of `hidden_one`, `qkv_proj`, `attended`, `hidden_two` and `activation`) count: a program that leaves them out, or rounds other values in their place, can miss the bound.
Values may be sent and summed in bfloat16 or wider, within the bound.
A program may use at most 320 MiB of HBM per device.

```python
import math
import jax
import jax.numpy as jnp
import numpy as np
from jax import lax

D = 1600
H = 25
HD = 64
FF = 6400
LEN = 1024
SEGS = 4
SEQUENCES = 4


def draw_block_input(key, part):
    noise = jax.random.normal(jax.random.fold_in(key, 21), (SEQUENCES, LEN, D), jnp.float32)
    return jnp.clip(noise, -8.0, 8.0).astype(jnp.bfloat16)


def draw_qkv_weight(key, part):
    normal_part = jax.random.normal(jax.random.fold_in(key, 31), (D, 3, H, HD), jnp.float32)
    base = jnp.clip(normal_part, -4.0, 4.0) * D ** (-0.5)
    return base.reshape(D, 3 * H * HD).astype(jnp.bfloat16)


def levels(stream_key, dims, pieces, least, largest):
    loudness = 1.0
    for axis_at, parts in pieces:
        heights = jax.random.uniform(jax.random.fold_in(jax.random.fold_in(stream_key, 6), axis_at), (parts,), jnp.float32, least / len(pieces), largest / len(pieces))
        loudness = loudness * jnp.repeat(jnp.exp(heights), dims[axis_at] // parts).reshape((-1,) + (1,) * (len(dims) - 1 - axis_at))
    return loudness


def split_up(count, total, most, slope):
    portions = [(1 << 20) // math.isqrt(standing ** slope) + 1 for standing in range(2, count + 1)]
    rest, holding = total - most - (count - 1), [1] * (count - 1)
    while rest > 0:
        free = [i for i in range(count - 1) if holding[i] < most]
        whole, remaining = sum([portions[i] for i in free]), rest
        for i in free:
            extra = min(most - holding[i], max(1, remaining * portions[i] // whole), rest)
            holding[i] = holding[i] + extra
            rest = rest - extra
    return np.array([most] + holding)


def uneven_parts(key, amount, total, bound, lean):
    if amount == 2:
        one = jax.random.randint(key, (), max(1, total - bound), min(bound, total - 1) + 1)
        return jnp.stack([one, total - one])
    lengths = jnp.asarray(split_up(amount, total, bound, lean), jnp.int32)
    pairs = (amount - 1) // 2
    source_of, sink = lengths[1:1 + 2 * pairs:2], lengths[2:2 + 2 * pairs:2]
    margin = jnp.minimum(source_of - 1, bound - sink)
    moved = jax.random.randint(jax.random.fold_in(key, 1), (pairs,), 0, 1 << 20) % (margin + 1)
    lengths = lengths.at[1:1 + 2 * pairs:2].set(source_of - moved).at[2:2 + 2 * pairs:2].set(sink + moved)
    return lengths[jax.random.permutation(jax.random.fold_in(key, 2), amount)]


def scatter_about(rng, dims, deviation, reach, cuts=(), dtype=jnp.bfloat16):
    loudness = levels(rng, dims, cuts, -0.22, 0.18) if cuts else 1.0
    entries = jax.random.normal(rng, dims, jnp.float32) * deviation * loudness
    return jnp.minimum(jnp.maximum(entries, -reach), reach).astype(dtype)


def setup_inputs(seed: int = 0) -> dict:
    streams_of = jax.random.split(jax.random.key(seed), 12)
    return {
        "block_input": draw_block_input(jax.random.fold_in(streams_of[11], 71), 0),
        "segments": jax.vmap(lambda own: jnp.searchsorted(jnp.cumsum(uneven_parts(own, SEGS, LEN, LEN // 2, 0)), jnp.arange(LEN), side="right"))(jax.random.split(streams_of[1], SEQUENCES)).reshape((SEQUENCES, LEN)).astype(jnp.int32),
        "ln1_gain": jnp.clip(1.0 + 0.1 * jax.random.normal(streams_of[2], (D,), jnp.float32), 0.5, 1.5),
        "ln1_shift": scatter_about(streams_of[3], (D,), 0.3, 3.0, (), jnp.float32),
        "qkv_weight": draw_qkv_weight(jax.random.fold_in(streams_of[11], 71), 0),
        "out_weight": scatter_about(streams_of[5], (H * HD, D), (D // 8) ** -0.5, 0.4375, ((1, 4),)),
        "ln2_gain": jnp.clip(1.0 + 0.1 * jax.random.normal(streams_of[6], (D,), jnp.float32), 0.5, 1.5),
        "ln2_shift": scatter_about(streams_of[7], (D,), 0.3, 3.0, (), jnp.float32),
        "fc_weight": scatter_about(streams_of[8], (D, FF), D ** -0.5, 0.15625, ((0, 4), (1, 2))),
        "proj_weight": scatter_about(streams_of[9], (FF, D), FF ** -0.5, 0.078125, ((0, 2), (1, 4))),
        "cotangent": scatter_about(streams_of[10], (SEQUENCES, LEN, D), 1.0, 6.0, ((0, 4), (1, 4))),
    }


norm_epsilon = 1e-05

@jax.custom_vjp
def low(v):
    return lax.optimization_barrier(v.astype(jnp.bfloat16)).astype(jnp.float32)

@jax.custom_vjp
def low_back(v):
    return v

def low_keep(v):
    return (low(v), None)

def low_pass(kept, grad):
    return (grad,)

def back_keep(v):
    return (v, None)

def back_low(kept, grad):
    return (low(grad),)
low.defvjp(low_keep, low_pass)
low_back.defvjp(back_keep, back_low)

def layer_norm(values, norm_gain, norm_shift):
    row_mean = lax.optimization_barrier(jnp.mean(values, axis=-1, keepdims=True))
    centered = values - row_mean
    variance = lax.optimization_barrier(jnp.mean(centered * centered, axis=-1, keepdims=True))
    return centered * lax.rsqrt(variance + norm_epsilon) * norm_gain + norm_shift

def attention(queries, key_rows, value_rows, seq_segments):
    raw_scores = low_back(jnp.einsum('qhd,khd->hqk', queries, key_rows, precision=lax.Precision.HIGHEST))
    scores = raw_scores * HD ** (-0.5)
    positions = jnp.arange(LEN)
    allowed = (positions[None, :] <= positions[:, None]) & (seq_segments[None, :] == seq_segments[:, None])
    scores = jnp.where(allowed[None], scores, -1e+30)
    probabilities = low(jax.nn.softmax(scores, axis=-1))
    attended = jnp.einsum('hqk,khd->qhd', probabilities, value_rows, precision=lax.Precision.HIGHEST)
    return low(low_back(attended)).reshape(LEN, H * HD)

def block(input_f32, seq_segments, gain_one, shift_one, query_key_value_weight, contract_weight, gain_two, shift_two, expand_weight, attention_projection_weight):
    highest = lax.Precision.HIGHEST
    hidden_one = low(layer_norm(input_f32, gain_one, shift_one))
    qkv_proj = low(low_back(jnp.dot(hidden_one, query_key_value_weight, precision=highest))).reshape(LEN, 3, H, HD)
    attended = jax.checkpoint(attention)(qkv_proj[:, 0], qkv_proj[:, 1], qkv_proj[:, 2], seq_segments)
    attn_sum = low_back(jnp.dot(attended, contract_weight, precision=highest))
    residual_one = input_f32 + attn_sum
    hidden_two = low(layer_norm(residual_one, gain_two, shift_two))
    pre_act = low_back(jnp.dot(hidden_two, expand_weight, precision=highest))
    activation = low(jax.nn.gelu(pre_act, approximate=True))
    mlp_sum = low_back(jnp.dot(activation, attention_projection_weight, precision=highest))
    return residual_one + mlp_sum

def reference(block_input, segments, ln1_gain, ln1_shift, qkv_weight, out_weight, ln2_gain, ln2_shift, fc_weight, proj_weight, cotangent):
    params_f32 = (ln1_gain.astype(jnp.float32), ln1_shift.astype(jnp.float32), qkv_weight.astype(jnp.float32), out_weight.astype(jnp.float32), ln2_gain.astype(jnp.float32), ln2_shift.astype(jnp.float32), fc_weight.astype(jnp.float32), proj_weight.astype(jnp.float32))

    def per_sequence(running, sequence_item):
        seq_input, seq_segments, seq_cotangent = sequence_item

        def forward(input_f32, gain_one, shift_one, query_key_value_weight, contract_weight, gain_two, shift_two, expand_weight, attention_projection_weight):
            return block(input_f32, seq_segments, gain_one, shift_one, query_key_value_weight, contract_weight, gain_two, shift_two, expand_weight, attention_projection_weight)
        result, pullback = jax.vjp(forward, seq_input.astype(jnp.float32), *params_f32)
        gradients = pullback(seq_cotangent.astype(jnp.float32))
        running = tuple((acc_term + grad_term for acc_term, grad_term in zip(running, gradients[1:])))
        return (running, (result.astype(jnp.bfloat16), gradients[0]))
    zero_sums = tuple((jnp.zeros_like(param) for param in params_f32))
    grad_totals, per_seq = lax.scan(per_sequence, zero_sums, (block_input, segments, cotangent))
    return (per_seq[0], per_seq[1], grad_totals[0], grad_totals[1], grad_totals[2], grad_totals[3], grad_totals[4], grad_totals[5], grad_totals[6], grad_totals[7])
```

```python
import jax
import jax.numpy as jnp
from jax import lax
from jax.sharding import PartitionSpec as P

H = 25
HD = 64
EPS = 1e-05
BF = jnp.bfloat16
F32 = jnp.float32
PLANE = ("ctx", "tp")


def dot(lhs, rhs, dims):
    return lax.dot_general(lhs, rhs, (dims, ((), ())), preferred_element_type=F32)


def moments(values):
    centered = values - jnp.mean(values, axis=-1, keepdims=True)
    inv_std = lax.rsqrt(jnp.mean(centered * centered, axis=-1, keepdims=True) + EPS)
    return centered * inv_std, inv_std


def norm_back(upstream, normed, inv_std, gain):
    scaled = upstream * gain
    return inv_std * (
        scaled
        - jnp.mean(scaled, axis=-1, keepdims=True)
        - normed * jnp.mean(scaled * normed, axis=-1, keepdims=True)
    )


def gelu_tanh(values):
    return jax.nn.gelu(values, approximate=True)


def masked_scores(queries, keys, seg):
    length = queries.shape[0]
    scores = jnp.einsum("qhd,khd->hqk", queries, keys, preferred_element_type=F32) * HD ** (-0.5)
    pos = jnp.arange(length, dtype=jnp.int32)
    allowed = (pos[None, :] <= pos[:, None]) & (seg[None, :] == seg[:, None])
    return jnp.where(allowed[None], scores, -1e30)


def attend(queries, keys, values, seg):
    scores = masked_scores(queries, keys, seg)
    row_max = jnp.max(scores, axis=-1, keepdims=True)
    exponent = jnp.exp(scores - row_max)
    total = jnp.sum(exponent, axis=-1, keepdims=True)
    probs = (exponent / total).astype(BF)
    attended = jnp.einsum("hqk,khd->qhd", probs, values, preferred_element_type=F32)
    return attended.astype(BF), row_max + jnp.log(total)


def attend_back(queries, keys, values, seg, lse, grad):
    probs = jnp.exp(masked_scores(queries, keys, seg) - lse)
    grad_v = jnp.einsum("hqk,qhd->khd", probs.astype(BF), grad, preferred_element_type=F32)
    grad_p = jnp.einsum("qhd,khd->hqk", grad, values, preferred_element_type=F32)
    inner = jnp.sum(probs * grad_p, axis=-1, keepdims=True)
    raw = (probs * (grad_p - inner) * HD ** (-0.5)).astype(BF)
    grad_q = jnp.einsum("hqk,khd->qhd", raw, keys, preferred_element_type=F32)
    grad_k = jnp.einsum("hqk,qhd->khd", raw, queries, preferred_element_type=F32)
    return grad_q, grad_k, grad_v


def build(mesh):
    ctx_n, tp_n = mesh.shape["ctx"], mesh.shape["tp"]
    members = ctx_n * tp_n
    slots = -(-H // members)
    starts = [m * H // members for m in range(members + 1)]
    counts = [starts[m + 1] - starts[m] for m in range(members)]
    width = slots * HD

    def local(x, segments, g1, b1, wqkv, wout, g2, b2, wfc, wproj, cot):
        x, cot = x[0], cot[0]
        rows, model = x.shape
        tp_i, ctx_i = lax.axis_index("tp"), lax.axis_index("ctx")
        member = ctx_i * tp_n + tp_i
        own = rows // tp_n
        head0 = member * H // members
        head_n = (member + 1) * H // members - head0
        valid = jnp.arange(width, dtype=jnp.int32) < head_n * HD

        def cols(matrix, start, size):
            return lax.dynamic_slice_in_dim(matrix, start, size, 1)

        def rows_of(matrix, start, size):
            return lax.dynamic_slice_in_dim(matrix, start, size, 0)

        wq = jnp.concatenate([cols(wqkv, p * H * HD + head0 * HD, width) for p in range(3)], axis=1)
        wq = lax.all_gather(wq, "fsdp", axis=0, tiled=True)
        part = model // members
        wo = lax.all_gather(rows_of(wout, member * part, part), "fsdp", axis=1, tiled=True)
        wo = lax.all_gather(wo, PLANE, axis=0, tiled=True)
        hidden = wfc.shape[1] // ctx_n
        wf = lax.all_gather(cols(wfc, ctx_i * hidden, hidden), "fsdp", axis=0, tiled=True)
        wp = lax.all_gather(rows_of(wproj, ctx_i * hidden, hidden), "fsdp", axis=1, tiled=True)

        def to_plane(v):
            return lax.all_gather(v, PLANE, axis=0, tiled=True)

        def from_plane(v):
            return lax.psum_scatter(v, PLANE, scatter_dimension=0, tiled=True)

        x_own = rows_of(x, tp_i * own, own)
        cot_own = rows_of(cot, tp_i * own, own)
        x_all = to_plane(x_own)
        cot_all = to_plane(cot_own)
        seg = lax.all_gather(segments[0], "ctx", axis=0, tiled=True)
        length = x_all.shape[0]

        n1_all, _ = moments(x_all.astype(F32))
        h1 = (n1_all * g1 + b1).astype(BF)
        qkv = dot(h1, wq, ((1,), (0,))).astype(BF).reshape(length, 3, slots, HD)
        q, k, v = qkv[:, 0], qkv[:, 1], qkv[:, 2]
        attended, lse = attend(q, k, v, seg)
        attended = attended.reshape(length, width)
        spread = lax.all_to_all(attended, PLANE, 0, 1, tiled=True)
        att_own = jnp.concatenate(
            [spread[:, m * width : m * width + counts[m] * HD] for m in range(members)], axis=1
        )
        x_own_f32 = x_own.astype(F32)
        r1 = x_own_f32 + dot(att_own, wo, ((1,), (0,)))
        n2, s2 = moments(r1)
        h2 = to_plane((n2 * g2 + b2).astype(BF))
        pre = dot(h2, wf, ((1,), (0,)))
        act, pull = jax.vjp(gelu_tanh, pre)
        act = act.astype(BF)
        mlp = from_plane(dot(act, wp, ((1,), (0,))))
        out = lax.all_gather((r1 + mlp).astype(BF), "tp", axis=0, tiled=True)

        grad_proj = dot(act, cot_all, ((0,), (0,)))
        grad_pre = pull(dot(cot_all, wp, ((1,), (1,))))[0].astype(BF)
        grad_fc = dot(h2, grad_pre, ((0,), (0,)))
        grad_h2 = from_plane(dot(grad_pre, wf, ((1,), (1,))))
        grad_r1 = cot_own.astype(F32) + norm_back(grad_h2, n2, s2, g2)
        grad_att = to_plane(grad_r1.astype(BF))
        wo_mine = rows_of(wo, head0 * HD, width)
        grad_out = dot(attended, grad_att, ((0,), (0,)))
        grad_attended = jnp.where(valid, dot(grad_att, wo_mine, ((1,), (1,))), 0.0).astype(BF)
        dq, dk, dv = attend_back(q, k, v, seg, lse, grad_attended.reshape(length, slots, HD))
        dqkv = jnp.stack([dq, dk, dv], axis=1).astype(BF).reshape(length, 3 * width)
        grad_qkv = dot(h1, dqkv, ((0,), (0,)))
        grad_h1 = from_plane(dot(dqkv, wq, ((1,), (1,))))
        n1, s1 = moments(x_own_f32)
        grad_x = grad_r1 + norm_back(grad_h1, n1, s1, g1)
        grad_x = lax.all_gather(grad_x, "tp", axis=0, tiled=True)

        def over_fsdp(v, dim):
            return lax.psum_scatter(v, "fsdp", scatter_dimension=dim, tiled=True)

        fc_out = lax.all_to_all(over_fsdp(grad_fc, 0), "ctx", 0, 1, tiled=True)
        proj_out = lax.all_to_all(over_fsdp(grad_proj, 1), "ctx", 1, 0, tiled=True)
        gq = over_fsdp(grad_qkv, 0).astype(BF)
        gq = gq.reshape(ctx_n, gq.shape[0] // ctx_n, 3 * width)
        gq = lax.all_gather(lax.all_to_all(gq, "ctx", 0, 0, tiled=True), "tp", axis=1)
        gq = gq.reshape((members,) + gq.shape[2:])
        qkv_out = jnp.concatenate(
            [
                gq[m][:, p * width : p * width + counts[m] * HD]
                for p in range(3)
                for m in range(members)
            ],
            axis=1,
        ).astype(F32)
        go = over_fsdp(grad_out, 1).astype(BF)
        go = lax.all_to_all(go, "ctx", 1, 0, tiled=True)
        go = lax.all_gather(go.reshape(ctx_n, width, go.shape[1]), "tp", axis=1)
        go = go.reshape((members,) + go.shape[2:])
        out_out = jnp.concatenate([go[m][: counts[m] * HD] for m in range(members)], axis=0)
        out_out = out_out.astype(F32)
        sums = jnp.stack(
            [
                jnp.sum(grad_h1 * n1, axis=0),
                jnp.sum(grad_h1, axis=0),
                jnp.sum(grad_h2 * n2, axis=0),
                jnp.sum(grad_h2, axis=0),
            ]
        )
        sums = lax.psum_scatter(
            lax.psum(sums, "tp"), ("fsdp", "ctx"), scatter_dimension=1, tiled=True
        )
        return (
            out[None],
            grad_x[None],
            sums[0],
            sums[1],
            qkv_out,
            out_out,
            sums[2],
            sums[3],
            fc_out,
            proj_out,
        )

    return local


def solution(mesh):
    placed = (
        P("fsdp", "ctx", None),
        P("fsdp", "ctx"),
        P(),
        P(),
        P("fsdp", None),
        P(None, "fsdp"),
        P(),
        P(),
        P("fsdp", "tp"),
        P("tp", "fsdp"),
        P("fsdp", "ctx", None),
    )
    both = ("fsdp", "ctx")
    return jax.shard_map(
        build(mesh),
        mesh=mesh,
        in_specs=placed,
        out_specs=(
            P("fsdp", "ctx", None),
            P("fsdp", "ctx", None),
            P(both),
            P(both),
            P(both, None),
            P(None, both),
            P(both),
            P(both),
            P(both, "tp"),
            P("tp", both),
        ),
        check_vma=False,
    )
```

```python
import functools

import jax
import jax.numpy as jnp
from jax import lax
from jax.experimental import pallas as pl
from jax.experimental.pallas import tpu as pltpu
from jax.sharding import PartitionSpec as P

H = 25
HD = 64
EPS = 1e-05
BF = jnp.bfloat16
F32 = jnp.float32
PLANE = ("ctx", "tp")


VMEM = pl.BlockSpec(memory_space=pltpu.VMEM)
MESH = pl.DeviceIdType.MESH


def flip(index, stride):
    return index + stride * (1 - 2 * ((index // stride) % 2))


def strides_of(ctx_n, tp_i):
    bits = ctx_n.bit_length() - 1
    plain = [1 << b for b in range(bits)]
    turned = plain[1:] + plain[:1]
    return [a + (b - a) * tp_i for a, b in zip(plain, turned)]


def greet(partners):
    barrier = pltpu.get_barrier_semaphore()
    for who in partners:
        pl.semaphore_signal(barrier, inc=1, device_id=who, device_id_type=MESH)
    pl.semaphore_wait(barrier, len(partners))


def remote(src, dst, send, recv, who):
    return pltpu.make_async_remote_copy(
        src_ref=src, dst_ref=dst, send_sem=send, recv_sem=recv, device_id=who, device_id_type=MESH
    )


def comm_params(ident, limit):
    return pltpu.CompilerParams(
        collective_id=ident, has_side_effects=True, vmem_limit_bytes=limit
    )


def gather_kernel(ctx_n, tp_n, own_ref, all_ref, send, recv, sib_send, sib_recv, local_sem):
    rows = own_ref.shape[0]
    ctx_i, tp_i = lax.axis_index("ctx"), lax.axis_index("tp")
    strides = strides_of(ctx_n, tp_i)
    sibling = {"tp": 1 - tp_i}
    greet([{"ctx": flip(ctx_i, s)} for s in strides] + [sibling])

    def place(c):
        return all_ref.at[pl.ds(pl.multiple_of((c * tp_n + tp_i) * rows, rows), rows)]

    mine = pltpu.make_async_copy(own_ref, place(ctx_i), local_sem)
    mine.start()
    held = [ctx_i]
    pending = []
    to_sibling = remote(own_ref, place(ctx_i), sib_send.at[0], sib_recv.at[0], sibling)
    to_sibling.start()
    pending.append(to_sibling)
    slot = 0
    for step, stride in enumerate(strides):
        copies = []
        for position, c in enumerate(held):
            src = own_ref if position == 0 else place(c)
            copy = remote(src, place(c), send.at[slot], recv.at[slot], {"ctx": flip(ctx_i, stride)})
            copy.start()
            copies.append(copy)
            slot += 1
        fresh = [flip(c, stride) for c in held]
        for copy, c in zip(copies, fresh):
            copy.wait_recv()
            passed = len(pending)
            onward = remote(place(c), place(c), sib_send.at[passed], sib_recv.at[passed], sibling)
            onward.start()
            pending.append(onward)
        for copy in copies:
            copy.wait_send()
        held = held + fresh
    for copy in pending:
        copy.wait()
    mine.wait()


def plane_gather(own, ctx_n, tp_n, ident):
    rows, columns = own.shape
    return pl.pallas_call(
        functools.partial(gather_kernel, ctx_n, tp_n),
        out_shape=jax.ShapeDtypeStruct((rows * ctx_n * tp_n, columns), own.dtype),
        in_specs=[VMEM],
        out_specs=VMEM,
        scratch_shapes=[
            pltpu.SemaphoreType.DMA((ctx_n - 1,)),
            pltpu.SemaphoreType.DMA((ctx_n - 1,)),
            pltpu.SemaphoreType.DMA((ctx_n,)),
            pltpu.SemaphoreType.DMA((ctx_n,)),
            pltpu.SemaphoreType.DMA,
        ],
        compiler_params=comm_params(ident, 32 << 20),
        cost_estimate=pl.CostEstimate(flops=0, bytes_accessed=30 << 20, transcendentals=0),
        name=f"plane_gather_{ident}",
    )(own)


def exchange_kernel(ctx_n, tp_n, src_ref, dst_ref, send, recv, local_sem):
    members = ctx_n * tp_n
    rows = src_ref.shape[0] // members
    me = lax.axis_index("ctx") * tp_n + lax.axis_index("tp")

    def block(member):
        return src_ref.at[pl.ds(pl.multiple_of(member * rows, rows), rows)]

    others = [lax.rem(me + shift, members) for shift in range(1, members)]
    ids = [{"ctx": other // tp_n, "tp": other % tp_n} for other in others]
    greet(ids)
    copies = [
        remote(block(other), dst_ref.at[me], send.at[i], recv.at[i], who)
        for i, (other, who) in enumerate(zip(others, ids))
    ]
    for copy in copies:
        copy.start()
    mine = pltpu.make_async_copy(block(me), dst_ref.at[me], local_sem)
    mine.start()
    for copy in copies:
        copy.wait()
    mine.wait()


def plane_exchange(values, ctx_n, tp_n, ident):
    members = ctx_n * tp_n
    rows, columns = values.shape
    return pl.pallas_call(
        functools.partial(exchange_kernel, ctx_n, tp_n),
        out_shape=jax.ShapeDtypeStruct((members, rows // members, columns), values.dtype),
        in_specs=[VMEM],
        out_specs=VMEM,
        scratch_shapes=[
            pltpu.SemaphoreType.DMA((members - 1,)),
            pltpu.SemaphoreType.DMA((members - 1,)),
            pltpu.SemaphoreType.DMA,
        ],
        compiler_params=comm_params(ident, 16 << 20),
        cost_estimate=pl.CostEstimate(flops=0, bytes_accessed=15 << 20, transcendentals=0),
        name=f"plane_exchange_{ident}",
    )(values)


def reduce_kernel(
    ctx_n, tp_n, turned, lhs_ref, rhs_ref, out_ref,
    part, near, got, sib_send, sib_recv, send, recv,
):
    rows = out_ref.shape[0]
    ctx_i, tp_i = lax.axis_index("ctx"), lax.axis_index("tp")
    strides = strides_of(ctx_n, tp_i)
    sibling = {"tp": 1 - tp_i}
    greet([{"ctx": flip(ctx_i, s)} for s in strides] + [sibling])
    contract = ((1,), (1,)) if turned else ((1,), (0,))
    to_sibling, onward = {}, {}
    bits = len(strides)

    def common(r):
        turn = sum(1 << ((b + 1) % bits) for b in range(bits) if r >> b & 1)
        return r + (turn - r) * tp_i

    def first(r):
        c = ctx_i
        for b, stride in enumerate(strides):
            if r >> b & 1:
                c = flip(c, stride)
        pair = lhs_ref[pl.ds(pl.multiple_of(c * tp_n * rows, tp_n * rows), tp_n * rows), :]
        part[r] = dot(pair, rhs_ref[...], contract).reshape(tp_n, rows, rhs_ref.shape[0 if turned else 1])
        to_sibling[r] = remote(
            part.at[r, 1 - tp_i], near.at[common(r)],
            sib_send.at[r], sib_recv.at[common(r)], sibling,
        )
        to_sibling[r].start()

    def second(r):
        to_sibling[r].wait_recv()
        total = part[r, tp_i] + near[common(r)]
        high = r.bit_length() - 1
        for b in range(high + 1, len(strides)):
            slot = (1 << b) - 1 + r
            onward[(1 << b) + r].wait_recv()
            total = total + got[slot]
        if r:
            near[common(r)] = total
            slot = r - 1
            onward[r] = remote(
                near.at[common(r)], got.at[slot], send.at[slot], recv.at[slot],
                {"ctx": flip(ctx_i, strides[high])},
            )
            onward[r].start()
        else:
            out_ref[...] = total

    order = list(range(ctx_n - 1, -1, -1))
    for i, r in enumerate(order):
        first(r)
        if i:
            second(order[i - 1])
    second(order[-1])
    for copy in list(to_sibling.values()) + list(onward.values()):
        copy.wait_send()


def plane_reduce(lhs, rhs, ctx_n, tp_n, turned, ident):
    members = ctx_n * tp_n
    rows = lhs.shape[0] // members
    columns = rhs.shape[0 if turned else 1]
    inner = lhs.shape[1]
    return pl.pallas_call(
        functools.partial(reduce_kernel, ctx_n, tp_n, turned),
        out_shape=jax.ShapeDtypeStruct((rows, columns), F32),
        in_specs=[VMEM, VMEM],
        out_specs=VMEM,
        scratch_shapes=[
            pltpu.VMEM((ctx_n, tp_n, rows, columns), F32),
            pltpu.VMEM((ctx_n, rows, columns), F32),
            pltpu.VMEM((ctx_n - 1, rows, columns), F32),
            pltpu.SemaphoreType.DMA((ctx_n,)),
            pltpu.SemaphoreType.DMA((ctx_n,)),
            pltpu.SemaphoreType.DMA((ctx_n - 1,)),
            pltpu.SemaphoreType.DMA((ctx_n - 1,)),
        ],
        compiler_params=comm_params(ident, 48 << 20),
        cost_estimate=pl.CostEstimate(
            flops=2 * lhs.shape[0] * inner * columns, bytes_accessed=60 << 20, transcendentals=0
        ),
        name=f"plane_reduce_{ident}",
    )(lhs, rhs)


def dot(lhs, rhs, dims):
    return lax.dot_general(lhs, rhs, (dims, ((), ())), preferred_element_type=F32)


def moments(values):
    centered = values - jnp.mean(values, axis=-1, keepdims=True)
    inv_std = lax.rsqrt(jnp.mean(centered * centered, axis=-1, keepdims=True) + EPS)
    return centered * inv_std, inv_std


def norm_back(upstream, normed, inv_std, gain):
    scaled = upstream * gain
    return inv_std * (
        scaled
        - jnp.mean(scaled, axis=-1, keepdims=True)
        - normed * jnp.mean(scaled * normed, axis=-1, keepdims=True)
    )


def gelu_tanh(values):
    return jax.nn.gelu(values, approximate=True)


def masked_scores(queries, keys, seg):
    length = queries.shape[0]
    scores = jnp.einsum("qhd,khd->hqk", queries, keys, preferred_element_type=F32) * HD ** (-0.5)
    pos = jnp.arange(length, dtype=jnp.int32)
    allowed = (pos[None, :] <= pos[:, None]) & (seg[None, :] == seg[:, None])
    return jnp.where(allowed[None], scores, -1e30)


def attend(queries, keys, values, seg):
    scores = masked_scores(queries, keys, seg)
    row_max = jnp.max(scores, axis=-1, keepdims=True)
    exponent = jnp.exp(scores - row_max)
    total = jnp.sum(exponent, axis=-1, keepdims=True)
    probs = (exponent / total).astype(BF)
    attended = jnp.einsum("hqk,khd->qhd", probs, values, preferred_element_type=F32)
    return attended.astype(BF), row_max + jnp.log(total)


def attend_back(queries, keys, values, seg, lse, grad):
    probs = jnp.exp(masked_scores(queries, keys, seg) - lse)
    grad_v = jnp.einsum("hqk,qhd->khd", probs.astype(BF), grad, preferred_element_type=F32)
    grad_p = jnp.einsum("qhd,khd->hqk", grad, values, preferred_element_type=F32)
    inner = jnp.sum(probs * grad_p, axis=-1, keepdims=True)
    raw = (probs * (grad_p - inner) * HD ** (-0.5)).astype(BF)
    grad_q = jnp.einsum("hqk,khd->qhd", raw, keys, preferred_element_type=F32)
    grad_k = jnp.einsum("hqk,qhd->khd", raw, queries, preferred_element_type=F32)
    return grad_q, grad_k, grad_v


def build(mesh):
    ctx_n, tp_n = mesh.shape["ctx"], mesh.shape["tp"]
    members = ctx_n * tp_n
    slots = -(-H // members)
    starts = [m * H // members for m in range(members + 1)]
    counts = [starts[m + 1] - starts[m] for m in range(members)]
    width = slots * HD

    def local(x, segments, g1, b1, wqkv, wout, g2, b2, wfc, wproj, cot):
        x, cot = x[0], cot[0]
        rows, model = x.shape
        tp_i, ctx_i = lax.axis_index("tp"), lax.axis_index("ctx")
        member = ctx_i * tp_n + tp_i
        own = rows // tp_n
        head0 = member * H // members
        head_n = (member + 1) * H // members - head0
        valid = jnp.arange(width, dtype=jnp.int32) < head_n * HD

        def cols(matrix, start, size):
            return lax.dynamic_slice_in_dim(matrix, start, size, 1)

        def rows_of(matrix, start, size):
            return lax.dynamic_slice_in_dim(matrix, start, size, 0)

        wq = jnp.concatenate([cols(wqkv, p * H * HD + head0 * HD, width) for p in range(3)], axis=1)
        wq = lax.all_gather(wq, "fsdp", axis=0, tiled=True)
        part = model // members
        wo = lax.all_gather(rows_of(wout, member * part, part), "fsdp", axis=1, tiled=True)
        wo = lax.all_gather(wo, PLANE, axis=0, tiled=True)
        hidden = wfc.shape[1] // ctx_n
        wf = lax.all_gather(cols(wfc, ctx_i * hidden, hidden), "fsdp", axis=0, tiled=True)
        wp = lax.all_gather(rows_of(wproj, ctx_i * hidden, hidden), "fsdp", axis=1, tiled=True)

        def to_plane(v, ident):
            return plane_gather(v, ctx_n, tp_n, ident)

        def from_plane(lhs, rhs, turned, ident):
            return plane_reduce(lhs, rhs, ctx_n, tp_n, turned, ident)

        x_own = rows_of(x, tp_i * own, own)
        cot_own = rows_of(cot, tp_i * own, own)
        x_all = to_plane(x_own, 0)
        cot_all = to_plane(cot_own, 1)
        seg = lax.all_gather(segments[0], "ctx", axis=0, tiled=True)
        length = x_all.shape[0]

        n1_all, _ = moments(x_all.astype(F32))
        h1 = (n1_all * g1 + b1).astype(BF)
        qkv = dot(h1, wq, ((1,), (0,))).astype(BF).reshape(length, 3, slots, HD)
        q, k, v = qkv[:, 0], qkv[:, 1], qkv[:, 2]
        attended, lse = attend(q, k, v, seg)
        attended = attended.reshape(length, width)
        spread = plane_exchange(attended, ctx_n, tp_n, 2)
        att_own = jnp.concatenate(
            [spread[m][:, : counts[m] * HD] for m in range(members)], axis=1
        )
        x_own_f32 = x_own.astype(F32)
        r1 = x_own_f32 + dot(att_own, wo, ((1,), (0,)))
        n2, s2 = moments(r1)
        h2 = to_plane((n2 * g2 + b2).astype(BF), 3)
        pre = dot(h2, wf, ((1,), (0,)))
        act, pull = jax.vjp(gelu_tanh, pre)
        act = act.astype(BF)
        mlp = lax.psum_scatter(
            dot(act, wp, ((1,), (0,))), PLANE, scatter_dimension=0, tiled=True
        )
        out = lax.all_gather((r1 + mlp).astype(BF), "tp", axis=0, tiled=True)

        grad_proj = dot(act, cot_all, ((0,), (0,)))
        grad_pre = pull(dot(cot_all, wp, ((1,), (1,))))[0].astype(BF)
        grad_fc = dot(h2, grad_pre, ((0,), (0,)))
        grad_h2 = from_plane(grad_pre, wf, True, 4)
        grad_r1 = cot_own.astype(F32) + norm_back(grad_h2, n2, s2, g2)
        grad_att = to_plane(grad_r1.astype(BF), 5)
        wo_mine = rows_of(wo, head0 * HD, width)
        grad_out = dot(attended, grad_att, ((0,), (0,)))
        grad_attended = jnp.where(valid, dot(grad_att, wo_mine, ((1,), (1,))), 0.0).astype(BF)
        dq, dk, dv = attend_back(q, k, v, seg, lse, grad_attended.reshape(length, slots, HD))
        dqkv = jnp.stack([dq, dk, dv], axis=1).astype(BF).reshape(length, 3 * width)
        grad_qkv = dot(h1, dqkv, ((0,), (0,)))
        grad_h1 = from_plane(dqkv, wq, True, 6)
        n1, s1 = moments(x_own_f32)
        grad_x = grad_r1 + norm_back(grad_h1, n1, s1, g1)
        grad_x = lax.all_gather(grad_x, "tp", axis=0, tiled=True)

        def over_fsdp(v, dim):
            return lax.psum_scatter(v, "fsdp", scatter_dimension=dim, tiled=True)

        fc_out = lax.all_to_all(over_fsdp(grad_fc, 0), "ctx", 0, 1, tiled=True)
        proj_out = lax.all_to_all(over_fsdp(grad_proj, 1), "ctx", 1, 0, tiled=True)
        gq = over_fsdp(grad_qkv, 0).astype(BF)
        gq = gq.reshape(ctx_n, gq.shape[0] // ctx_n, 3 * width)
        gq = lax.all_gather(lax.all_to_all(gq, "ctx", 0, 0, tiled=True), "tp", axis=1)
        gq = gq.reshape((members,) + gq.shape[2:])
        qkv_out = jnp.concatenate(
            [
                gq[m][:, p * width : p * width + counts[m] * HD]
                for p in range(3)
                for m in range(members)
            ],
            axis=1,
        ).astype(F32)
        go = over_fsdp(grad_out, 1).astype(BF)
        go = lax.all_to_all(go, "ctx", 1, 0, tiled=True)
        go = lax.all_gather(go.reshape(ctx_n, width, go.shape[1]), "tp", axis=1)
        go = go.reshape((members,) + go.shape[2:])
        out_out = jnp.concatenate([go[m][: counts[m] * HD] for m in range(members)], axis=0)
        out_out = out_out.astype(F32)
        sums = jnp.stack(
            [
                jnp.sum(grad_h1 * n1, axis=0),
                jnp.sum(grad_h1, axis=0),
                jnp.sum(grad_h2 * n2, axis=0),
                jnp.sum(grad_h2, axis=0),
            ]
        )
        share = model // (lax.axis_size("fsdp") * ctx_n)
        place = lax.axis_index("fsdp") * ctx_n + ctx_i
        sums = cols(lax.psum(sums, ("fsdp", "ctx", "tp")), place * share, share)
        return (
            out[None],
            grad_x[None],
            sums[0],
            sums[1],
            qkv_out,
            out_out,
            sums[2],
            sums[3],
            fc_out,
            proj_out,
        )

    return local


def solution(mesh):
    placed = (
        P("fsdp", "ctx", None),
        P("fsdp", "ctx"),
        P(),
        P(),
        P("fsdp", None),
        P(None, "fsdp"),
        P(),
        P(),
        P("fsdp", "tp"),
        P("tp", "fsdp"),
        P("fsdp", "ctx", None),
    )
    both = ("fsdp", "ctx")
    return jax.shard_map(
        build(mesh),
        mesh=mesh,
        in_specs=placed,
        out_specs=(
            P("fsdp", "ctx", None),
            P("fsdp", "ctx", None),
            P(both),
            P(both),
            P(both, None),
            P(None, both),
            P(both),
            P(both),
            P(both, "tp"),
            P("tp", both),
        ),
        check_vma=False,
    )
```

```python
import functools

import jax
import jax.numpy as jnp
from jax import lax
from jax.experimental import pallas as pl
from jax.experimental.pallas import tpu as pltpu
from jax.sharding import PartitionSpec as P


H = 25
HD = 64
EPS = 1e-05
BF = jnp.bfloat16
F32 = jnp.float32
HALF_FLOAT = jnp.float16


VMEM = pl.BlockSpec(memory_space=pltpu.VMEM)
MESH = pl.DeviceIdType.MESH


def flip(index, stride):
    return index + stride * (1 - 2 * ((index // stride) % 2))


def strides_of(ctx_n, tp_i):
    bits = ctx_n.bit_length() - 1
    plain = [1 << b for b in range(bits)]
    turned = plain[1:] + plain[:1]
    return [a + (b - a) * tp_i for a, b in zip(plain, turned)]


def greet(partners):
    barrier = pltpu.get_barrier_semaphore()
    for who in partners:
        pl.semaphore_signal(barrier, inc=1, device_id=who, device_id_type=MESH)
    pl.semaphore_wait(barrier, len(partners))


def remote(src, dst, send, recv, who):
    return pltpu.make_async_remote_copy(
        src_ref=src, dst_ref=dst, send_sem=send, recv_sem=recv, device_id=who, device_id_type=MESH
    )


def comm_params(ident, limit):
    return pltpu.CompilerParams(
        collective_id=ident, has_side_effects=True, vmem_limit_bytes=limit
    )


def gather_kernel(ctx_n, tp_n, count, *refs):
    owns, alls = refs[:count], refs[count : 2 * count]
    send, recv, sib_send, sib_recv, local_sem = refs[2 * count :]
    ctx_i, tp_i = lax.axis_index("ctx"), lax.axis_index("tp")
    strides = strides_of(ctx_n, tp_i)
    sibling = {"tp": 1 - tp_i}
    greet([{"ctx": flip(ctx_i, s)} for s in strides] + [sibling])
    pending = []

    def place(n, c):
        rows = owns[n].shape[0]
        return alls[n].at[pl.ds(pl.multiple_of((c * tp_n + tp_i) * rows, rows), rows)]

    def pass_on(n, source, c, which):
        copy = remote(source, place(n, c), sib_send.at[n, which], sib_recv.at[n, which], sibling)
        copy.start()
        pending.append(copy)

    mine = [pltpu.make_async_copy(owns[n], place(n, ctx_i), local_sem.at[n]) for n in range(count)]
    held, slot = [ctx_i], 0
    for stride in strides:
        partner = {"ctx": flip(ctx_i, stride)}
        copies = []
        for position, c in enumerate(held):
            for n in range(count):
                source = owns[n] if position == 0 else place(n, c)
                copy = remote(source, place(n, c), send.at[n, slot], recv.at[n, slot], partner)
                copy.start()
                copies.append((copy, n, slot + 1, flip(c, stride)))
            slot += 1
        if len(held) == 1:
            for n in range(count):
                mine[n].start()
                pass_on(n, owns[n], ctx_i, 0)
        for copy, n, which, fresh in copies:
            copy.wait_recv()
            pass_on(n, place(n, fresh), fresh, which)
        for copy, _, _, _ in copies:
            copy.wait_send()
        held = held + [flip(c, stride) for c in held]
    for copy in pending + mine:
        copy.wait()


def plane_gather(owns, ctx_n, tp_n, ident):
    count = len(owns)
    return pl.pallas_call(
        functools.partial(gather_kernel, ctx_n, tp_n, count),
        out_shape=tuple(
            jax.ShapeDtypeStruct((own.shape[0] * ctx_n * tp_n, own.shape[1]), own.dtype)
            for own in owns
        ),
        in_specs=[VMEM] * count,
        out_specs=(VMEM,) * count,
        scratch_shapes=[
            pltpu.SemaphoreType.DMA((count, ctx_n - 1)),
            pltpu.SemaphoreType.DMA((count, ctx_n - 1)),
            pltpu.SemaphoreType.DMA((count, ctx_n)),
            pltpu.SemaphoreType.DMA((count, ctx_n)),
            pltpu.SemaphoreType.DMA((count,)),
        ],
        compiler_params=comm_params(ident, 24 << 20),
        cost_estimate=pl.CostEstimate(flops=0, bytes_accessed=30 << 20, transcendentals=0),
    )(*owns)


def sum_kernel(mesh_shape, tiles_ref, out_ref, got, send, recv):
    fsdp_n, ctx_n, tp_n = mesh_shape
    total = fsdp_n * ctx_n * tp_n
    me = (lax.axis_index("fsdp") * ctx_n + lax.axis_index("ctx")) * tp_n + lax.axis_index("tp")
    others = [lax.rem(me + shift, total) for shift in range(1, total)]
    ids = [
        {"fsdp": o // (ctx_n * tp_n), "ctx": (o // tp_n) % ctx_n, "tp": o % tp_n} for o in others
    ]
    greet(ids)
    copies = []
    for i, (other, who) in enumerate(zip(others, ids)):
        copy = remote(tiles_ref.at[other // tp_n], got.at[i], send.at[i], recv.at[i], who)
        copy.start()
        copies.append(copy)
    value = tiles_ref[me // tp_n]
    for i, copy in enumerate(copies):
        copy.wait_recv()
        value = value + got[i]
    out_ref[...] = value
    for copy in copies:
        copy.wait_send()


def sum_everywhere(rows, mesh_shape, ident):
    fsdp_n, ctx_n, tp_n = mesh_shape
    places = fsdp_n * ctx_n
    share = rows.shape[1] // places
    tiles = jnp.transpose(rows.reshape(rows.shape[0], places, share), (1, 0, 2))
    tiles = jnp.pad(tiles, ((0, 0), (0, 8 - rows.shape[0]), (0, 128 - share)))
    total = pl.pallas_call(
        functools.partial(sum_kernel, mesh_shape),
        out_shape=jax.ShapeDtypeStruct((8, 128), F32),
        in_specs=[VMEM],
        out_specs=VMEM,
        scratch_shapes=[
            pltpu.VMEM((places * tp_n - 1, 8, 128), F32),
            pltpu.SemaphoreType.DMA((places * tp_n - 1,)),
            pltpu.SemaphoreType.DMA((places * tp_n - 1,)),
        ],
        compiler_params=comm_params(ident, 8 << 20),
        cost_estimate=pl.CostEstimate(flops=0, bytes_accessed=15 << 20, transcendentals=0),
        name="sum_everywhere",
    )(tiles)
    return total[: rows.shape[0], :share]


def reduce_kernel(
    ctx_n, tp_n, turned, lhs_ref, rhs_ref, out_ref,
    part, near, got, sib_send, sib_recv, send, recv,
):
    rows = out_ref.shape[0]
    ctx_i, tp_i = lax.axis_index("ctx"), lax.axis_index("tp")
    strides = strides_of(ctx_n, tp_i)
    sibling = {"tp": 1 - tp_i}
    greet([{"ctx": flip(ctx_i, s)} for s in strides] + [sibling])
    contract = ((1,), (1,)) if turned else ((1,), (0,))
    to_sibling, onward = {}, {}
    bits = len(strides)

    def common(r):
        turn = sum(1 << ((b + 1) % bits) for b in range(bits) if r >> b & 1)
        return r + (turn - r) * tp_i

    def first(r):
        c = ctx_i
        for b, stride in enumerate(strides):
            if r >> b & 1:
                c = flip(c, stride)
        pair = lhs_ref[pl.ds(pl.multiple_of(c * tp_n * rows, tp_n * rows), tp_n * rows), :]
        part[r] = dot(pair, rhs_ref[...], contract).reshape(tp_n, rows, rhs_ref.shape[0 if turned else 1])
        to_sibling[r] = remote(
            part.at[r, 1 - tp_i], near.at[common(r)],
            sib_send.at[r], sib_recv.at[common(r)], sibling,
        )
        to_sibling[r].start()

    def second(r):
        to_sibling[r].wait_recv()
        total = part[r, tp_i] + near[common(r)]
        high = r.bit_length() - 1
        for b in range(high + 1, len(strides)):
            slot = (1 << b) - 1 + r
            onward[(1 << b) + r].wait_recv()
            total = total + got[slot]
        if r:
            near[common(r)] = total
            slot = r - 1
            onward[r] = remote(
                near.at[common(r)], got.at[slot], send.at[slot], recv.at[slot],
                {"ctx": flip(ctx_i, strides[high])},
            )
            onward[r].start()
        else:
            out_ref[...] = total

    order = list(range(ctx_n - 1, -1, -1))
    for i, r in enumerate(order):
        first(r)
        if i:
            second(order[i - 1])
    second(order[-1])
    for copy in list(to_sibling.values()) + list(onward.values()):
        copy.wait_send()


def plane_reduce(lhs, rhs, ctx_n, tp_n, turned, ident):
    members = ctx_n * tp_n
    rows = lhs.shape[0] // members
    columns = rhs.shape[0 if turned else 1]
    inner = lhs.shape[1]
    return pl.pallas_call(
        functools.partial(reduce_kernel, ctx_n, tp_n, turned),
        out_shape=jax.ShapeDtypeStruct((rows, columns), F32),
        in_specs=[VMEM, VMEM],
        out_specs=VMEM,
        scratch_shapes=[
            pltpu.VMEM((ctx_n, tp_n, rows, columns), F32),
            pltpu.VMEM((ctx_n, rows, columns), F32),
            pltpu.VMEM((ctx_n - 1, rows, columns), F32),
            pltpu.SemaphoreType.DMA((ctx_n,)),
            pltpu.SemaphoreType.DMA((ctx_n,)),
            pltpu.SemaphoreType.DMA((ctx_n - 1,)),
            pltpu.SemaphoreType.DMA((ctx_n - 1,)),
        ],
        compiler_params=comm_params(ident, 48 << 20),
        cost_estimate=pl.CostEstimate(
            flops=2 * lhs.shape[0] * inner * columns, bytes_accessed=60 << 20, transcendentals=0
        ),
    )(lhs, rhs)


def dot(lhs, rhs, dims):
    return lax.dot_general(lhs, rhs, (dims, ((), ())), preferred_element_type=F32)


def moments(values):
    centered = values - jnp.mean(values, axis=-1, keepdims=True)
    inv_std = lax.rsqrt(jnp.mean(centered * centered, axis=-1, keepdims=True) + EPS)
    return centered * inv_std, inv_std


def norm_back(upstream, normed, inv_std, gain):
    scaled = upstream * gain
    return inv_std * (
        scaled
        - jnp.mean(scaled, axis=-1, keepdims=True)
        - normed * jnp.mean(scaled * normed, axis=-1, keepdims=True)
    )


HALF = 2 * HD


def mask_bias(seg_row_ref, seg_col_ref, i, j, block):
    same = seg_col_ref[pl.ds(j * block, block), :] == seg_row_ref[:, pl.ds(i * block, block)]
    if i == j:
        key = lax.broadcasted_iota(jnp.int32, (block, block), 0)
        query = lax.broadcasted_iota(jnp.int32, (block, block), 1)
        same = same & (key <= query)
    return same


def attend_kernel(block, q_ref, k_ref, v_ref, row_ref, col_ref, out_ref, lse_ref, qt, vt, ot, s_ref):
    length = q_ref.shape[0]
    qt[...] = q_ref[...].T
    vt[...] = v_ref[...].T
    for h in range(2):
        head = slice(h * HD, (h + 1) * HD)
        for i in range(length // block):
            cols = slice(i * block, (i + 1) * block)
            row_max = None
            for j in range(i + 1):
                s = dot(k_ref[j * block : (j + 1) * block, head], qt[head, cols], ((1,), (0,)))
                s = jnp.where(mask_bias(row_ref, col_ref, i, j, block), s * HD ** (-0.5), -1e30)
                s_ref[j * block : (j + 1) * block, :] = s
                top = jnp.max(s, axis=0, keepdims=True)
                row_max = top if row_max is None else jnp.maximum(row_max, top)
            total = jnp.zeros((1, block), F32)
            for j in range(i + 1):
                e = jnp.exp(s_ref[j * block : (j + 1) * block, :] - row_max)
                s_ref[j * block : (j + 1) * block, :] = e
                total = total + jnp.sum(e, axis=0, keepdims=True)
            scale = 1.0 / total
            acc = jnp.zeros((HD, block), F32)
            for j in range(i + 1):
                p = (s_ref[j * block : (j + 1) * block, :] * scale).astype(BF)
                acc = acc + dot(vt[head, j * block : (j + 1) * block], p, ((1,), (0,)))
            ot[head, cols] = acc
            lse_ref[0, h : h + 1, cols] = row_max + jnp.log(total)
    out_ref[...] = ot[...].T.astype(BF)


def attention(qkv, seg, slots):
    length = qkv.shape[0]
    pairs = slots // 2
    block = min(256, length)
    return pl.pallas_call(
        functools.partial(attend_kernel, block),
        grid=(pairs,),
        out_shape=(
            jax.ShapeDtypeStruct((length, slots * HD), BF),
            jax.ShapeDtypeStruct((pairs, 2, length), F32),
        ),
        in_specs=[
            pl.BlockSpec((length, HALF), lambda p: (0, p)),
            pl.BlockSpec((length, HALF), lambda p: (0, pairs + p)),
            pl.BlockSpec((length, HALF), lambda p: (0, 2 * pairs + p)),
            pl.BlockSpec((1, length), lambda p: (0, 0)),
            pl.BlockSpec((length, 1), lambda p: (0, 0)),
        ],
        out_specs=(
            pl.BlockSpec((length, HALF), lambda p: (0, p)),
            pl.BlockSpec((1, 2, length), lambda p: (p, 0, 0)),
        ),
        scratch_shapes=[
            pltpu.VMEM((HALF, length), BF),
            pltpu.VMEM((HALF, length), BF),
            pltpu.VMEM((HALF, length), F32),
            pltpu.VMEM((length, block), F32),
        ],
        compiler_params=pltpu.CompilerParams(vmem_limit_bytes=24 << 20),
        cost_estimate=pl.CostEstimate(
            flops=4 * length * length * slots * HD, bytes_accessed=40 << 20, transcendentals=0
        ),
        name="attend",
    )(qkv, qkv, qkv, seg[None, :], seg[:, None])


def attend_back_kernel(
    block, pairs, q_ref, k_ref, v_ref, g_ref, lse_ref, row_ref, col_ref, out_ref,
    qt, kt, gt, dqt, dkt, dvt, p_ref, dp_ref,
):
    length = q_ref.shape[0]
    scale = HD ** (-0.5)
    qt[...] = q_ref[...].T
    kt[...] = k_ref[...].T
    gt[...] = g_ref[...].T
    for h in range(2):
        head = slice(h * HD, (h + 1) * HD)
        for i in range(length // block):
            cols = slice(i * block, (i + 1) * block)
            lse = lse_ref[0, h : h + 1, cols]
            inner = jnp.zeros((1, block), F32)
            for j in range(i + 1):
                keys = slice(j * block, (j + 1) * block)
                s = dot(k_ref[keys, head], qt[head, cols], ((1,), (0,))) * scale
                s = jnp.where(mask_bias(row_ref, col_ref, i, j, block), s, -1e30)
                p = jnp.exp(s - lse)
                dp = dot(v_ref[keys, head], gt[head, cols], ((1,), (0,)))
                inner = inner + jnp.sum(p * dp, axis=0, keepdims=True)
                p_ref[keys, :] = p
                dp_ref[keys, :] = dp
                dv = dot(gt[head, cols], p.astype(BF), ((1,), (1,)))
                dvt[head, keys] = dv if i == j else dvt[head, keys] + dv
            acc = jnp.zeros((HD, block), F32)
            for j in range(i + 1):
                keys = slice(j * block, (j + 1) * block)
                ds = (p_ref[keys, :] * (dp_ref[keys, :] - inner) * scale).astype(BF)
                acc = acc + dot(kt[head, keys], ds, ((1,), (0,)))
                dk = dot(qt[head, cols], ds, ((1,), (1,)))
                dkt[head, keys] = dk if i == j else dkt[head, keys] + dk
            dqt[head, cols] = acc
    pair = pl.program_id(0)
    for part, ref in enumerate((dqt, dkt, dvt)):
        start = pl.multiple_of((part * pairs + pair) * HALF, HALF)
        out_ref[:, pl.ds(start, HALF)] = ref[...].T.astype(BF)


def attention_back(qkv, grad, lse, seg, slots):
    length = qkv.shape[0]
    pairs = slots // 2
    block = min(256, length)
    return pl.pallas_call(
        functools.partial(attend_back_kernel, block, pairs),
        grid=(pairs,),
        out_shape=jax.ShapeDtypeStruct((length, 3 * slots * HD), BF),
        in_specs=[
            pl.BlockSpec((length, HALF), lambda p: (0, p)),
            pl.BlockSpec((length, HALF), lambda p: (0, pairs + p)),
            pl.BlockSpec((length, HALF), lambda p: (0, 2 * pairs + p)),
            pl.BlockSpec((length, HALF), lambda p: (0, p)),
            pl.BlockSpec((1, 2, length), lambda p: (p, 0, 0)),
            pl.BlockSpec((1, length), lambda p: (0, 0)),
            pl.BlockSpec((length, 1), lambda p: (0, 0)),
        ],
        out_specs=pl.BlockSpec((length, 3 * slots * HD), lambda p: (0, 0)),
        scratch_shapes=[
            pltpu.VMEM((HALF, length), BF),
            pltpu.VMEM((HALF, length), BF),
            pltpu.VMEM((HALF, length), BF),
            pltpu.VMEM((HALF, length), F32),
            pltpu.VMEM((HALF, length), F32),
            pltpu.VMEM((HALF, length), F32),
            pltpu.VMEM((length, block), F32),
            pltpu.VMEM((length, block), F32),
        ],
        compiler_params=pltpu.CompilerParams(vmem_limit_bytes=32 << 20),
        cost_estimate=pl.CostEstimate(
            flops=10 * length * length * slots * HD, bytes_accessed=80 << 20, transcendentals=0
        ),
        name="attend_back",
    )(qkv, qkv, qkv, grad, lse, seg[None, :], seg[:, None])


def weight_grad_kernel(fsdp_n, lhs_ref, rhs_ref, own_ref, *refs):
    sent, full = refs[: fsdp_n - 1], refs[fsdp_n - 1]
    rows, columns = own_ref.shape
    me = lax.axis_index("fsdp")
    tops = []
    step = rows if rows % 128 else 4 * 128
    for r in range(0, full.shape[0], step):
        part = slice(r, min(r + step, full.shape[0]))
        value = dot(lhs_ref[:, part], rhs_ref[...], ((0,), (0,)))
        full[part, :] = value
        tops.append(jnp.max(jnp.abs(value)))
    top = jnp.full((1, columns), functools.reduce(jnp.maximum, tops))
    exponent = jnp.floor(jnp.log2(jnp.maximum(top, 1e-30)))
    scale = jnp.exp2(14.0 - exponent)

    def block(index):
        return full[pl.ds(pl.multiple_of(index * rows, rows), rows), :]

    own_ref[...] = block(me)
    for s, ref in enumerate(sent, 1):
        ref[:rows, :] = block(lax.rem(me + s, fsdp_n)) * scale
        ref[rows:, :] = jnp.broadcast_to(exponent, (ref.shape[0] - rows, columns))


def weight_grad(lhs, rhs, fsdp_n):
    rows, columns = lhs.shape[1] // fsdp_n, rhs.shape[1]
    blocks = pl.pallas_call(
        functools.partial(weight_grad_kernel, fsdp_n),
        out_shape=(jax.ShapeDtypeStruct((rows, columns), F32),)
        + (jax.ShapeDtypeStruct((rows + 16, columns), F32),) * (fsdp_n - 1),
        in_specs=[VMEM, VMEM],
        out_specs=(VMEM,) * fsdp_n,
        scratch_shapes=[pltpu.VMEM((lhs.shape[1], columns), F32)],
        compiler_params=pltpu.CompilerParams(vmem_limit_bytes=30 << 20),
        cost_estimate=pl.CostEstimate(
            flops=2 * lhs.shape[0] * lhs.shape[1] * columns,
            bytes_accessed=20 << 20,
            transcendentals=0,
        ),
        name="weight_grad",
    )(lhs, rhs)
    arrived = {}
    for shift in sorted(range(1, fsdp_n), key=lambda v: min(v, fsdp_n - v)):
        arrived[shift] = lax.ppermute(
            blocks[shift].astype(HALF_FLOAT),
            "fsdp",
            [(i, (i + shift) % fsdp_n) for i in range(fsdp_n)],
        )

    def finish(dtype=F32):
        total = blocks[0]
        for block_in in arrived.values():
            back = jnp.exp2(block_in[rows, 0].astype(F32) - 14.0)
            total = total + block_in[:rows].astype(F32) * back
        return total.astype(dtype)

    return finish


GELU_A = (2.0 / jnp.pi) ** 0.5
GELU_B = 0.044715


def activate_kernel(h_ref, w_ref, pre_ref, act_ref):
    u = dot(h_ref[...], w_ref[...], ((1,), (0,)))
    pre_ref[...] = u
    act_ref[...] = (0.5 * u * (1.0 + jnp.tanh(GELU_A * (u + GELU_B * (u * u * u))))).astype(BF)


def activate_back_kernel(g_ref, w_ref, pre_ref, out_ref):
    upstream = dot(g_ref[...], w_ref[...], ((1,), (0,)))
    u = pre_ref[...]
    t = jnp.tanh(GELU_A * (u + GELU_B * (u * u * u)))
    slope = 0.5 * (1.0 + t) + 0.5 * u * (1.0 - t * t) * (GELU_A * (1.0 + 3.0 * GELU_B * (u * u)))
    out_ref[...] = (upstream * slope).astype(BF)


def row_blocks(kernel, lhs, rhs, others, out_dtypes):
    length, inner = lhs.shape
    columns = rhs.shape[1]
    block = min(256, length)
    wide = pl.BlockSpec((block, columns), lambda i: (i, 0))
    return pl.pallas_call(
        kernel,
        grid=(length // block,),
        out_shape=tuple(jax.ShapeDtypeStruct((length, columns), d) for d in out_dtypes),
        in_specs=[
            pl.BlockSpec((block, inner), lambda i: (i, 0)),
            pl.BlockSpec((inner, columns), lambda i: (0, 0)),
        ]
        + [wide] * len(others),
        out_specs=(wide,) * len(out_dtypes),
        compiler_params=pltpu.CompilerParams(vmem_limit_bytes=24 << 20),
        cost_estimate=pl.CostEstimate(
            flops=2 * length * inner * columns, bytes_accessed=20 << 20, transcendentals=0
        ),
    )(lhs, rhs, *others)


def place_kernel(ctx_n, tp_n, counts, src_ref, out_ref, got, send, recv, sib_send, sib_recv, local_sem):
    ctx_i, tp_i = lax.axis_index("ctx"), lax.axis_index("tp")
    sibling = {"tp": 1 - tp_i}
    others = [lax.rem(ctx_i + shift, ctx_n) for shift in range(1, ctx_n)]
    greet([{"ctx": c} for c in others] + [sibling])
    me = ctx_i * tp_n + tp_i
    copies = []
    for i, c in enumerate(others):
        copy = remote(src_ref.at[c], got.at[me], send.at[i], recv.at[i], {"ctx": c})
        copy.start()
        copies.append(copy)
    passed = [remote(src_ref.at[ctx_i], got.at[me], sib_send.at[0], sib_recv.at[0], sibling)]
    passed[0].start()
    mine = pltpu.make_async_copy(src_ref.at[ctx_i], got.at[me], local_sem)
    mine.start()
    for i, copy in enumerate(copies):
        copy.wait_recv()
        source = lax.rem(ctx_i + ctx_n - 1 - i, ctx_n) * tp_n + tp_i
        onward = remote(
            got.at[source], got.at[source], sib_send.at[i + 1], sib_recv.at[i + 1], sibling
        )
        onward.start()
        passed.append(onward)
    for copy in passed:
        copy.wait_recv()
    mine.wait()
    rows = out_ref.shape[0]
    width = src_ref.shape[2] // 3
    start = 0
    for p in range(3):
        for m, count in enumerate(counts):
            size = count * HD
            out_ref[:, start : start + size] = got[m, :rows, p * width : p * width + size].astype(F32)
            start += size
    for copy in copies + passed:
        copy.wait_send()


def place_heads(piece, ctx_n, tp_n, counts, ident):
    rows, columns = piece.shape[0] // ctx_n, piece.shape[1]
    members = ctx_n * tp_n
    tall = -(-rows // 16) * 16
    piece = jnp.pad(piece.reshape(ctx_n, rows, columns), ((0, 0), (0, tall - rows), (0, 0)))
    return pl.pallas_call(
        functools.partial(place_kernel, ctx_n, tp_n, counts),
        out_shape=jax.ShapeDtypeStruct((rows, 3 * sum(counts) * HD), F32),
        in_specs=[VMEM],
        out_specs=VMEM,
        scratch_shapes=[
            pltpu.VMEM((members, tall, columns), BF),
            pltpu.SemaphoreType.DMA((ctx_n - 1,)),
            pltpu.SemaphoreType.DMA((ctx_n - 1,)),
            pltpu.SemaphoreType.DMA((ctx_n,)),
            pltpu.SemaphoreType.DMA((ctx_n,)),
            pltpu.SemaphoreType.DMA,
        ],
        compiler_params=comm_params(ident, 16 << 20),
        cost_estimate=pl.CostEstimate(flops=0, bytes_accessed=20 << 20, transcendentals=0),
    )(piece)


def build(mesh):
    fsdp_n, ctx_n, tp_n = mesh.shape["fsdp"], mesh.shape["ctx"], mesh.shape["tp"]
    members = ctx_n * tp_n
    slots = 2 * -(-H // (2 * members))
    starts = [m * H // members for m in range(members + 1)]
    counts = [starts[m + 1] - starts[m] for m in range(members)]
    width = slots * HD

    def body(x, segments, g1, b1, wqkv, wout, g2, b2, wfc, wproj, cot):
        x, cot = x[0], cot[0]
        rows, model = x.shape
        tp_i, ctx_i = lax.axis_index("tp"), lax.axis_index("ctx")
        member = ctx_i * tp_n + tp_i
        own = rows // tp_n
        head0 = member * H // members
        head_n = (member + 1) * H // members - head0
        valid = jnp.arange(width, dtype=jnp.int32) < head_n * HD

        def cols(matrix, start, size):
            return lax.dynamic_slice_in_dim(matrix, start, size, 1)

        def rows_of(matrix, start, size):
            return lax.dynamic_slice_in_dim(matrix, start, size, 0)

        hidden = wfc.shape[1] // ctx_n
        wo = jnp.where(valid, rows_of(wout, head0 * HD, width).T, jnp.zeros((), BF))
        heads = [cols(wqkv, p * H * HD + head0 * HD, width) for p in range(3)]
        first = lax.all_gather(jnp.concatenate(heads + [wo], axis=1), "fsdp", axis=0, tiled=True)
        wq, wo = first[:, : 3 * width], first[:, 3 * width :]
        second = jnp.stack(
            [cols(wfc, ctx_i * hidden, hidden), rows_of(wproj, ctx_i * hidden, hidden).T]
        )
        second = lax.all_gather(second, "fsdp", axis=0)
        wf = second[:, 0].reshape(model, hidden)
        wp = second[:, 1].reshape(model, hidden)

        x_own = rows_of(x, tp_i * own, own)
        cot_own = rows_of(cot, tp_i * own, own)
        seg_own = jnp.broadcast_to(cols(segments, tp_i * own, own), (8, own))
        x_all, seg, cot_all = plane_gather((x_own, seg_own, cot_own), ctx_n, tp_n, 0)
        length = x_all.shape[0]
        seg = seg.reshape(members, 8, own)[:, 0].reshape(length)

        n1_all, _ = moments(x_all.astype(F32))
        h1 = (n1_all * g1 + b1).astype(BF)
        qkv = dot(h1, wq, ((1,), (0,))).astype(BF)
        attended, lse = attention(qkv, seg, slots)
        x_own_f32 = x_own.astype(F32)
        r1 = x_own_f32 + plane_reduce(attended, wo, ctx_n, tp_n, True, 1)
        n2, s2 = moments(r1)
        (h2,) = plane_gather(((n2 * g2 + b2).astype(BF),), ctx_n, tp_n, 2)
        pre, act = row_blocks(activate_kernel, h2, wf, (), (F32, BF))
        proj_sum = weight_grad(cot_all, act, fsdp_n)
        (grad_pre,) = row_blocks(activate_back_kernel, cot_all, wp, (pre,), (BF,))
        fc_sum = weight_grad(h2, grad_pre, fsdp_n)
        grad_h2 = plane_reduce(grad_pre, wf, ctx_n, tp_n, True, 3)
        grad_r1 = cot_own.astype(F32) + norm_back(grad_h2, n2, s2, g2)
        (grad_att,) = plane_gather((grad_r1.astype(BF),), ctx_n, tp_n, 4)
        out_sum = weight_grad(grad_att, attended, fsdp_n)
        grad_attended = dot(grad_att, wo, ((1,), (0,))).astype(BF)
        dqkv = attention_back(qkv, grad_attended, lse, seg, slots)
        qkv_sum = weight_grad(h1, dqkv, fsdp_n)
        late, _ = lax.optimization_barrier((act, dqkv))
        mlp = plane_reduce(late, wp, ctx_n, tp_n, True, 7)
        out = lax.all_gather((r1 + mlp).astype(BF), "tp", axis=0, tiled=True)
        grad_h1 = plane_reduce(dqkv, wq, ctx_n, tp_n, True, 5)
        n1, s1 = moments(x_own_f32)
        grad_x = grad_r1 + norm_back(grad_h1, n1, s1, g1)
        grad_x = lax.all_gather(grad_x, "tp", axis=0, tiled=True)

        def to_places(v):
            return lax.all_to_all(v.reshape(ctx_n, -1, v.shape[1]), "ctx", 0, 0, tiled=True)

        def side_by_side(v):
            return jnp.moveaxis(v, 0, 1).reshape(v.shape[1], -1)

        def of_members(v):
            v = lax.all_gather(to_places(v), "tp", axis=1)
            return v.reshape((members,) + v.shape[2:]).astype(F32)

        fc_out = side_by_side(to_places(fc_sum()))
        proj_out = side_by_side(to_places(proj_sum())).T
        go = of_members(out_sum(BF))
        out_out = jnp.concatenate(
            [go[m][:, : counts[m] * HD] for m in range(members)], axis=1
        ).T
        qkv_out = place_heads(qkv_sum(BF), ctx_n, tp_n, counts, 8)
        sums = jnp.stack(
            [
                jnp.sum(grad_h1 * n1, axis=0),
                jnp.sum(grad_h1, axis=0),
                jnp.sum(grad_h2 * n2, axis=0),
                jnp.sum(grad_h2, axis=0),
            ]
        )
        sums = sum_everywhere(sums, (fsdp_n, ctx_n, tp_n), 6)
        return (
            out[None],
            grad_x[None],
            sums[0],
            sums[1],
            qkv_out,
            out_out,
            sums[2],
            sums[3],
            fc_out,
            proj_out,
        )

    return body


def solution(mesh):
    placed = (
        P("fsdp", "ctx", None),
        P("fsdp", "ctx"),
        P(),
        P(),
        P("fsdp", None),
        P(None, "fsdp"),
        P(),
        P(),
        P("fsdp", "tp"),
        P("tp", "fsdp"),
        P("fsdp", "ctx", None),
    )
    both = ("fsdp", "ctx")
    return jax.shard_map(
        build(mesh),
        mesh=mesh,
        in_specs=placed,
        out_specs=(
            P("fsdp", "ctx", None),
            P("fsdp", "ctx", None),
            P(both),
            P(both),
            P(both, None),
            P(None, both),
            P(both),
            P(both),
            P(both, "tp"),
            P("tp", both),
        ),
        check_vma=False,
    )
```
